8 devices in a mesh: dp: 8 (over z, y, x, core).
Axes of the slice: x: 2, y: 2, z: 1, core: 2. Of those that a mesh axis runs over, the one named last changes fastest.
Arguments:
- x_saved: bfloat16 [16, 768, 2048], P('dp')
- grad_out: bfloat16 [16, 768, 2048], P('dp')
- positions: int32 [16, 768], P('dp')
- attn_gain: bfloat16 [2048], replicated
- w_query: bfloat16 [2048, 16, 128], replicated
- w_key: bfloat16 [2048, 16, 128], replicated
- w_value: bfloat16 [2048, 16, 128], replicated
- w_out: bfloat16 [16, 128, 2048], replicated
- mlp_gain: bfloat16 [2048], replicated
- w_gate: bfloat16 [2048, 5504], replicated
- w_up: bfloat16 [2048, 5504], replicated
- w_down: bfloat16 [5504, 2048], replicated
- master_flat: float32 [50597888], P('dp')
- adam_mean: float32 [50597888], P('dp')
- adam_var: float32 [50597888], P('dp')
Outputs:
- output 1: bfloat16 [16, 768, 2048], P('dp')
- output 2: bfloat16 [2048], replicated
- output 3: bfloat16 [2048, 16, 128], replicated
- output 4: bfloat16 [2048, 16, 128], replicated
- output 5: bfloat16 [2048, 16, 128], replicated
- output 6: bfloat16 [16, 128, 2048], replicated
- output 7: bfloat16 [2048], replicated
- output 8: bfloat16 [2048, 5504], replicated
- output 9: bfloat16 [2048, 5504], replicated
- output 10: bfloat16 [5504, 2048], replicated
- output 11: float32 [50597888], P('dp')
- output 12: float32 [50597888], P('dp')
- output 13: float32 [50597888], P('dp')
- output 14: float32 [], replicated
All inputs are finite; a program needn't handle non-finite values.
Results may differ from the reference program's by a relative error of at most 0.0125245.
Values are sent between devices in bfloat16 or wider.
A program may use at most 1.5 GiB of HBM per device.

```python
import math
import jax
import jax.numpy as jnp
from jax import lax

MODEL_DIM = 2048
NUM_HEADS = 16
KV_HEADS = 16
HEAD_DIM = 128
FFN_DIM = 5504
SEQ_LEN = 768
SEQS_DEV = 2
DP_SIZE = 8
STEP_COUNT = 100
TOTAL_SEQS = SEQS_DEV * DP_SIZE
NPARAM = MODEL_DIM * (2 + 2 * HEAD_DIM * (NUM_HEADS + KV_HEADS) + 3 * FFN_DIM)
NORM_EPS = 1e-5
ROPE_BASE = 10000.0
LEARN_RATE = 2e-3
BETA_ONE = 0.9
BETA_TWO = 0.95
ADAM_EPS = 1e-8
WEIGHT_DECAY = 0.1


def param_shapes():
    return [(MODEL_DIM,), (MODEL_DIM, NUM_HEADS, HEAD_DIM), (MODEL_DIM, KV_HEADS, HEAD_DIM),
            (MODEL_DIM, KV_HEADS, HEAD_DIM), (NUM_HEADS, HEAD_DIM, MODEL_DIM), (MODEL_DIM,),
            (MODEL_DIM, FFN_DIM), (MODEL_DIM, FFN_DIM), (FFN_DIM, MODEL_DIM)]


def draw_params(key):
    key_list = jax.random.split(key, 9)
    fan_ins = [0, MODEL_DIM, MODEL_DIM, MODEL_DIM, NUM_HEADS * HEAD_DIM, 0, MODEL_DIM, MODEL_DIM, FFN_DIM]
    drawn_list = []
    for number, piece_shape in enumerate(param_shapes()):
        noise_arr = jax.random.normal(key_list[number], piece_shape, jnp.float32)
        if fan_ins[number] == 0:
            drawn_list.append(1.0 + 0.2 * noise_arr)
        else:
            drawn_list.append(noise_arr * fan_ins[number] ** -0.5)
    return drawn_list


def setup_inputs(seed: int = 0) -> dict:
    key_list = jax.random.split(jax.random.key(seed), 8)
    act_shape = (TOTAL_SEQS, SEQ_LEN, MODEL_DIM)
    x_saved = jax.random.normal(key_list[0], act_shape, jnp.float32).astype(jnp.bfloat16)
    grad_out = jax.random.normal(key_list[1], act_shape, jnp.float32).astype(jnp.bfloat16)
    pos_gaps = jax.random.randint(key_list[2], (TOTAL_SEQS, SEQ_LEN), 1, 4)
    positions = (jnp.cumsum(pos_gaps, axis=1) - 1).astype(jnp.int32)
    weights = [w_piece.astype(jnp.bfloat16) for w_piece in draw_params(key_list[3])]
    master_flat = jnp.concatenate([w_piece.reshape(-1) for w_piece in draw_params(key_list[4])])
    state_scale = NPARAM ** -0.5
    adam_mean = 0.1 * state_scale * jax.random.normal(key_list[5], (NPARAM,), jnp.float32)
    var_root = 0.3 * state_scale * jax.random.uniform(key_list[6], (NPARAM,), jnp.float32, 0.5, 1.5)
    adam_var = var_root * var_root
    return {'x_saved': x_saved, 'grad_out': grad_out, 'positions': positions,
            'attn_gain': weights[0], 'w_query': weights[1], 'w_key': weights[2], 'w_value': weights[3],
            'w_out': weights[4], 'mlp_gain': weights[5], 'w_gate': weights[6], 'w_up': weights[7],
            'w_down': weights[8], 'master_flat': master_flat, 'adam_mean': adam_mean, 'adam_var': adam_var}


def rms_scale(values, gain):
    wide = values.astype(jnp.float32)
    inv_rms = lax.rsqrt(jnp.mean(wide * wide, axis=-1, keepdims=True) + NORM_EPS)
    return (wide * inv_rms * gain.astype(jnp.float32)).astype(jnp.bfloat16)


def rope_tables(positions, head_dim):
    half_dim = head_dim // 2
    inv_freq = ROPE_BASE ** (-2.0 * jnp.arange(half_dim, dtype=jnp.float32) / head_dim)
    angles = positions.astype(jnp.float32)[:, :, None] * inv_freq
    cos_full = jnp.concatenate([jnp.cos(angles), jnp.cos(angles)], axis=-1)[:, :, None, :]
    sin_full = jnp.concatenate([jnp.sin(angles), jnp.sin(angles)], axis=-1)[:, :, None, :]
    return cos_full, sin_full


def rope_apply(values, cos_full, sin_full):
    half_dim = values.shape[-1] // 2
    rotated = jnp.concatenate([-values[..., half_dim:], values[..., :half_dim]], axis=-1)
    return values * cos_full + rotated * sin_full


def layer_forward(w_list, x_val, positions):
    attn_gain, w_query, w_key, w_value, w_out, mlp_gain, w_gate, w_up, w_down = w_list
    num_seqs, seq_len, model_dim = x_val.shape
    num_heads, head_dim = w_query.shape[1], w_query.shape[2]
    kv_heads = w_key.shape[1]
    group_size = num_heads // kv_heads
    n_tok = num_seqs * seq_len
    x_flat = x_val.reshape(n_tok, model_dim)
    normed = rms_scale(x_flat, attn_gain)
    q_pre = jnp.dot(normed, w_query.reshape(model_dim, num_heads * head_dim), preferred_element_type=jnp.float32)
    k_pre = jnp.dot(normed, w_key.reshape(model_dim, kv_heads * head_dim), preferred_element_type=jnp.float32)
    v_pre = jnp.dot(normed, w_value.reshape(model_dim, kv_heads * head_dim), preferred_element_type=jnp.float32)
    v_heads = v_pre.astype(jnp.bfloat16).reshape(num_seqs, seq_len, kv_heads, head_dim)
    cos_full, sin_full = rope_tables(positions, head_dim)
    q_rot = rope_apply(q_pre.reshape(num_seqs, seq_len, num_heads, head_dim), cos_full, sin_full).astype(jnp.bfloat16)
    q_rot = q_rot.reshape(num_seqs, seq_len, kv_heads, group_size, head_dim)
    k_rot = rope_apply(k_pre.reshape(num_seqs, seq_len, kv_heads, head_dim), cos_full, sin_full).astype(jnp.bfloat16)
    scores = jnp.einsum('bqkgd,bskd->bkgqs', q_rot.astype(jnp.float32), k_rot.astype(jnp.float32)) * head_dim ** -0.5
    causal = jnp.arange(seq_len)[:, None] >= jnp.arange(seq_len)[None, :]
    attn_probs = jax.nn.softmax(jnp.where(causal, scores, -1e30), axis=-1).astype(jnp.bfloat16)
    context = jnp.einsum('bkgqs,bskd->bqkgd', attn_probs.astype(jnp.float32), v_heads.astype(jnp.float32)).astype(jnp.bfloat16)
    attn_out = jnp.dot(context.reshape(n_tok, num_heads * head_dim), w_out.reshape(num_heads * head_dim, model_dim), preferred_element_type=jnp.float32)
    hidden = (x_flat.astype(jnp.float32) + attn_out).astype(jnp.bfloat16)
    normed_mlp = rms_scale(hidden, mlp_gain)
    gate_pre = jnp.dot(normed_mlp, w_gate, preferred_element_type=jnp.float32)
    up_pre = jnp.dot(normed_mlp, w_up, preferred_element_type=jnp.float32)
    gated_act = (jax.nn.silu(gate_pre) * up_pre).astype(jnp.bfloat16)
    down_out = jnp.dot(gated_act, w_down, preferred_element_type=jnp.float32)
    return (hidden.astype(jnp.float32) + down_out).astype(jnp.bfloat16).reshape(num_seqs, seq_len, model_dim)


def split_flat(flat_vec):
    pieces = []
    offset = 0
    for piece_shape in param_shapes():
        piece_size = math.prod(piece_shape)
        pieces.append(flat_vec[offset:offset + piece_size].reshape(piece_shape))
        offset += piece_size
    return pieces


def reference(x_saved, grad_out, positions, attn_gain, w_query, w_key, w_value, w_out, mlp_gain, w_gate, w_up, w_down, master_flat, adam_mean, adam_var):
    w_list = (attn_gain, w_query, w_key, w_value, w_out, mlp_gain, w_gate, w_up, w_down)

    def device_grads(grad_acc, group_in):
        x_group, dy_group, pos_group = group_in
        layer_out, pullback = jax.vjp(lambda x_val, w_vals: layer_forward(w_vals, x_val, pos_group), x_group, w_list)
        grad_x, grad_w = pullback(dy_group)
        flat_grad = jnp.concatenate([w_grad.astype(jnp.bfloat16).reshape(-1).astype(jnp.float32) for w_grad in grad_w])
        return grad_acc + flat_grad, grad_x.astype(jnp.bfloat16)

    group_shape = (DP_SIZE, SEQS_DEV, SEQ_LEN, MODEL_DIM)
    grad_sum, grad_x = lax.scan(device_grads, jnp.zeros((NPARAM,), jnp.float32),
                                (x_saved.reshape(group_shape), grad_out.reshape(group_shape),
                                 positions.reshape(DP_SIZE, SEQS_DEV, SEQ_LEN)))
    grad_mean = grad_sum / DP_SIZE
    grad_norm = jnp.sqrt(jnp.sum(grad_mean * grad_mean))
    clip_scale = jnp.minimum(1.0, 1.0 / (grad_norm + 1e-6))
    clipped = grad_mean * clip_scale
    new_mean = BETA_ONE * adam_mean + (1.0 - BETA_ONE) * clipped
    new_var = BETA_TWO * adam_var + (1.0 - BETA_TWO) * clipped * clipped
    mean_hat = new_mean / (1.0 - BETA_ONE ** STEP_COUNT)
    var_hat = new_var / (1.0 - BETA_TWO ** STEP_COUNT)
    gain_two = MODEL_DIM + 2 * MODEL_DIM * HEAD_DIM * (NUM_HEADS + KV_HEADS)
    flat_index = jnp.arange(NPARAM)
    is_gain = (flat_index < MODEL_DIM) | ((flat_index >= gain_two) & (flat_index < gain_two + MODEL_DIM))
    decays = jnp.where(is_gain, 0.0, WEIGHT_DECAY)
    new_master = master_flat - LEARN_RATE * (mean_hat / (jnp.sqrt(var_hat) + ADAM_EPS) + decays * master_flat)
    new_weights = split_flat(new_master.astype(jnp.bfloat16))
    return (grad_x.reshape(TOTAL_SEQS, SEQ_LEN, MODEL_DIM), new_weights[0], new_weights[1], new_weights[2],
            new_weights[3], new_weights[4], new_weights[5], new_weights[6], new_weights[7], new_weights[8],
            new_master, new_mean, new_var, grad_norm)
```

```python
import functools

import jax
import jax.numpy as jnp
import numpy as np
from jax import lax
from jax.experimental import pallas as pl
from jax.experimental.pallas import tpu as pltpu
from jax.sharding import PartitionSpec as P

NORM_EPS = 1e-5
ROPE_BASE = 10000.0
LEARN_RATE = 2e-3
BETA_ONE = 0.9
BETA_TWO = 0.95
ADAM_EPS = 1e-8
WEIGHT_DECAY = 0.1
STEP_COUNT = 100


def rope_tables(positions, head_dim):
    half_dim = head_dim // 2
    inv_freq = ROPE_BASE ** (-2.0 * jnp.arange(half_dim, dtype=jnp.float32) / head_dim)
    angles = positions.astype(jnp.float32)[:, :, None] * inv_freq
    cos_full = jnp.concatenate([jnp.cos(angles), jnp.cos(angles)], axis=-1)[:, :, None, :]
    sin_full = jnp.concatenate([jnp.sin(angles), jnp.sin(angles)], axis=-1)[:, :, None, :]
    return cos_full, sin_full


def rope_apply(values, cos_full, sin_full):
    half_dim = values.shape[-1] // 2
    rotated = jnp.concatenate([-values[..., half_dim:], values[..., :half_dim]], axis=-1)
    return values * cos_full + rotated * sin_full


def rope_back(grad_rot, cos_full, sin_full):
    half_dim = grad_rot.shape[-1] // 2
    scaled = grad_rot * sin_full
    return grad_rot * cos_full + jnp.concatenate([scaled[..., half_dim:], -scaled[..., :half_dim]], axis=-1)


def rms_parts(values):
    inv_rms = lax.rsqrt(jnp.mean(values * values, axis=-1, keepdims=True) + NORM_EPS)
    return inv_rms, values * inv_rms


def rms_back(d_normed, gain_wide, inv_rms, x_hat):
    d_hat = d_normed * gain_wide
    return inv_rms * (d_hat - x_hat * jnp.mean(d_hat * x_hat, axis=-1, keepdims=True))


def local_grads(x_loc, dy_loc, pos_loc, w_list):
    attn_gain, w_query, w_key, w_value, w_out, mlp_gain, w_gate, w_up, w_down = w_list
    num_seqs, seq_len, model_dim = x_loc.shape
    num_heads, head_dim = w_query.shape[1], w_query.shape[2]
    kv_heads = w_key.shape[1]
    group_size = num_heads // kv_heads
    n_tok = num_seqs * seq_len
    wq_flat = w_query.reshape(model_dim, num_heads * head_dim)
    wk_flat = w_key.reshape(model_dim, kv_heads * head_dim)
    wv_flat = w_value.reshape(model_dim, kv_heads * head_dim)
    wo_flat = w_out.reshape(num_heads * head_dim, model_dim)
    dy_flat = dy_loc.reshape(n_tok, model_dim)
    x_wide = x_loc.reshape(n_tok, model_dim).astype(jnp.float32)
    inv_one, value_a8 = rms_parts(x_wide)
    gain_one = attn_gain.astype(jnp.float32)
    normed = (value_a8 * gain_one).astype(jnp.bfloat16)
    q_pre = jnp.dot(normed, wq_flat, preferred_element_type=jnp.float32).reshape(num_seqs, seq_len, num_heads, head_dim)
    k_pre = jnp.dot(normed, wk_flat, preferred_element_type=jnp.float32).reshape(num_seqs, seq_len, kv_heads, head_dim)
    v_heads = jnp.dot(normed, wv_flat, preferred_element_type=jnp.float32).astype(jnp.bfloat16).reshape(num_seqs, seq_len, kv_heads, head_dim)
    cos_full, sin_full = rope_tables(pos_loc, head_dim)
    q_rot = rope_apply(q_pre, cos_full, sin_full).astype(jnp.bfloat16).reshape(num_seqs, seq_len, kv_heads, group_size, head_dim)
    k_rot = rope_apply(k_pre, cos_full, sin_full).astype(jnp.bfloat16)
    score_scale = head_dim ** -0.5
    scores = jnp.einsum('bqkgd,bskd->bkgqs', q_rot, k_rot, preferred_element_type=jnp.float32) * score_scale
    causal = lax.iota(jnp.int32, seq_len)[:, None] >= lax.iota(jnp.int32, seq_len)[None, :]
    attn_probs = jax.nn.softmax(jnp.where(causal, scores, -1e30), axis=-1)
    probs_low = attn_probs.astype(jnp.bfloat16)
    context = jnp.einsum('bkgqs,bskd->bqkgd', probs_low, v_heads, preferred_element_type=jnp.float32).astype(jnp.bfloat16)
    context = context.reshape(n_tok, num_heads * head_dim)
    attn_out = jnp.dot(context, wo_flat, preferred_element_type=jnp.float32)
    hidden = (x_wide + attn_out).astype(jnp.bfloat16)
    inv_two, array_b8 = rms_parts(hidden.astype(jnp.float32))
    gain_two = mlp_gain.astype(jnp.float32)
    normed_mlp = (array_b8 * gain_two).astype(jnp.bfloat16)
    gate_pre = jnp.dot(normed_mlp, w_gate, preferred_element_type=jnp.float32)
    up_pre = jnp.dot(normed_mlp, w_up, preferred_element_type=jnp.float32)
    gate_sig = jax.nn.sigmoid(gate_pre)
    gate_act = gate_pre * gate_sig
    gated_act = (gate_act * up_pre).astype(jnp.bfloat16)
    g_down = jnp.einsum('nf,nd->fd', gated_act, dy_flat, preferred_element_type=jnp.float32)
    d_gated = jnp.einsum('nd,fd->nf', dy_flat, w_down, preferred_element_type=jnp.float32)
    d_up = (d_gated * gate_act).astype(jnp.bfloat16)
    d_gate = (d_gated * up_pre * gate_sig * (1.0 + gate_pre * (1.0 - gate_sig))).astype(jnp.bfloat16)
    g_gate = jnp.einsum('nd,nf->df', normed_mlp, d_gate, preferred_element_type=jnp.float32)
    g_up = jnp.einsum('nd,nf->df', normed_mlp, d_up, preferred_element_type=jnp.float32)
    d_normed_mlp = (jnp.einsum('nf,df->nd', d_gate, w_gate, preferred_element_type=jnp.float32)
                    + jnp.einsum('nf,df->nd', d_up, w_up, preferred_element_type=jnp.float32))
    g_mlp_gain = jnp.sum(d_normed_mlp * array_b8, axis=0)
    d_hidden = rms_back(d_normed_mlp, gain_two, inv_two, array_b8) + dy_flat.astype(jnp.float32)
    d_hidden_low = d_hidden.astype(jnp.bfloat16)
    g_out = jnp.einsum('nc,nd->cd', context, d_hidden_low, preferred_element_type=jnp.float32)
    d_context = jnp.einsum('nd,cd->nc', d_hidden_low, wo_flat, preferred_element_type=jnp.float32).astype(jnp.bfloat16)
    d_context = d_context.reshape(num_seqs, seq_len, kv_heads, group_size, head_dim)
    d_probs = jnp.einsum('bqkgd,bskd->bkgqs', d_context, v_heads, preferred_element_type=jnp.float32)
    g_values = jnp.einsum('bkgqs,bqkgd->bskd', probs_low, d_context, preferred_element_type=jnp.float32)
    d_scores = (attn_probs * (d_probs - jnp.sum(d_probs * attn_probs, axis=-1, keepdims=True)) * score_scale).astype(jnp.bfloat16)
    d_q_rot = jnp.einsum('bkgqs,bskd->bqkgd', d_scores, k_rot, preferred_element_type=jnp.float32).reshape(num_seqs, seq_len, num_heads, head_dim)
    d_k_rot = jnp.einsum('bkgqs,bqkgd->bskd', d_scores, q_rot, preferred_element_type=jnp.float32)
    d_q_pre = rope_back(d_q_rot, cos_full, sin_full).astype(jnp.bfloat16).reshape(n_tok, num_heads * head_dim)
    d_k_pre = rope_back(d_k_rot, cos_full, sin_full).astype(jnp.bfloat16).reshape(n_tok, kv_heads * head_dim)
    d_v_pre = g_values.astype(jnp.bfloat16).reshape(n_tok, kv_heads * head_dim)
    g_query = jnp.einsum('nd,nc->dc', normed, d_q_pre, preferred_element_type=jnp.float32)
    g_key = jnp.einsum('nd,nc->dc', normed, d_k_pre, preferred_element_type=jnp.float32)
    g_value = jnp.einsum('nd,nc->dc', normed, d_v_pre, preferred_element_type=jnp.float32)
    d_normed = (jnp.einsum('nc,dc->nd', d_q_pre, wq_flat, preferred_element_type=jnp.float32)
                + jnp.einsum('nc,dc->nd', d_k_pre, wk_flat, preferred_element_type=jnp.float32)
                + jnp.einsum('nc,dc->nd', d_v_pre, wv_flat, preferred_element_type=jnp.float32))
    g_attn_gain = jnp.sum(d_normed * value_a8, axis=0)
    d_x = rms_back(d_normed, gain_one, inv_one, value_a8) + d_hidden
    grad_list = [g_attn_gain, g_query, g_key, g_value, g_out, g_mlp_gain, g_gate, g_up, g_down]
    return d_x.astype(jnp.bfloat16).reshape(num_seqs, seq_len, model_dim), grad_list


LANES = 128
SLAB_ROWS = 49412
CHUNK_ROWS = 12384
NUM_CHUNKS = 4
STEP_ROWS = 4128
SUB_ROWS = 32
GRAD_ROWS = NUM_CHUNKS * CHUNK_ROWS + 16
CARRY_ROWS = 704
ROW_BASE = {'wq': 16, 'wk': 32784, 'wv': 65552, 'wo': 98320, 'wg': 131104, 'wu': 219168, 'wd': 307232}
ROW_COUNT = {'wq': 32768, 'wk': 32768, 'wv': 32768, 'wo': 32768, 'wg': 88064, 'wu': 88064, 'wd': 88064}
GROUP_ROWS = {'wq': 256, 'wk': 256, 'wv': 256, 'wo': 256, 'wg': 688, 'wu': 688, 'wd': 256}
NAMES = ('wq', 'wk', 'wv', 'wo', 'wg', 'wu', 'wd')
GAIN_TWO_ROW = 131088


def frame_start(owner):
    return SLAB_ROWS * owner // 16 * 16


def frame_stop(owner):
    return -(-SLAB_ROWS * (owner + 1) // 16) * 16


def pieces_of(src):
    found = []
    for number, name in enumerate(NAMES):
        rows = ROW_COUNT[name] // 8
        start = ROW_BASE[name] + src * rows
        for owner in range(8):
            low, high = max(start, frame_start(owner)), min(start + rows, frame_stop(owner))
            if low < high:
                found.append((number, owner, low - start, low - frame_start(owner), high - low))
    return found


def regroup_kernel(*refs):
    shard_refs = refs[:7]
    gain_ref, sumsq_ref = refs[7:9]
    grad_ref, gains_out, sums_out = refs[9:12]
    bounce, gains_in, sums_in, send_sem, recv_sem, small_send, small_recv, local_sem = refs[12:]
    me = lax.axis_index('dp')

    def piece_copy(number, owner, src, src_row, dst_row, rows, slot):
        return pltpu.make_async_remote_copy(
            src_ref=shard_refs[number].at[pl.ds(src_row, rows), :],
            dst_ref=grad_ref.at[pl.ds(dst_row, rows), :],
            send_sem=send_sem.at[slot], recv_sem=recv_sem.at[number, src],
            device_id=(owner,), device_id_type=pl.DeviceIdType.MESH)

    def small_copy(src_ref, dst_ref, number, shift):
        return pltpu.make_async_remote_copy(
            src_ref=src_ref, dst_ref=dst_ref.at[me],
            send_sem=small_send.at[number, shift], recv_sem=small_recv.at[number, shift],
            device_id=(lax.rem(me + shift, 8),), device_id_type=pl.DeviceIdType.MESH)

    for shift in range(1, 8):
        small_copy(gain_ref, gains_in, 0, shift).start()
        small_copy(sumsq_ref, sums_in, 1, shift).start()
    all_pieces = [pieces_of(src) for src in range(8)]
    for src in range(8):
        @pl.when(me == src)
        def _():
            for slot, (number, owner, src_row, dst_row, rows) in enumerate(all_pieces[src]):
                if owner != src:
                    piece_copy(number, owner, src, src_row, dst_row, rows, slot).start()
            for number, owner, src_row, dst_row, rows in all_pieces[src]:
                if owner == src:
                    part = bounce.at[pl.ds(0, rows), :]
                    copy_in = pltpu.make_async_copy(shard_refs[number].at[pl.ds(src_row, rows), :], part, local_sem)
                    copy_in.start()
                    copy_in.wait()
                    copy_out = pltpu.make_async_copy(part, grad_ref.at[pl.ds(dst_row, rows), :], local_sem)
                    copy_out.start()
                    copy_out.wait()
    gains_in[me] = gain_ref[...]
    sums_in[me] = sumsq_ref[...]
    for shift in range(1, 8):
        small_copy(gain_ref, gains_in, 0, shift).wait()
        small_copy(sumsq_ref, sums_in, 1, shift).wait()
    gains_out[...] = gains_in[...]
    sums_out[...] = sums_in[...]
    for dev in range(8):
        @pl.when(me == dev)
        def _():
            for slot, (number, owner, src_row, dst_row, rows) in enumerate(all_pieces[dev]):
                if owner != dev:
                    piece_copy(number, owner, dev, src_row, dst_row, rows, slot).wait_send()
            for src in range(8):
                for number, owner, src_row, dst_row, rows in all_pieces[src]:
                    if owner == dev and src != dev:
                        piece_copy(number, owner, src, src_row, dst_row, rows, 0).wait_recv()


def regroup(shards, gain_rows, sumsq):
    any_spec = pl.BlockSpec(memory_space=pl.ANY)
    vmem_spec = pl.BlockSpec(memory_space=pltpu.VMEM)
    return pl.pallas_call(
        regroup_kernel,
        out_shape=(jax.ShapeDtypeStruct((GRAD_ROWS, LANES), jnp.bfloat16),
                   jax.ShapeDtypeStruct((8, 32, LANES), jnp.bfloat16),
                   jax.ShapeDtypeStruct((8, 8, LANES), jnp.float32)),
        in_specs=[any_spec] * 7 + [vmem_spec] * 2,
        out_specs=(any_spec, vmem_spec, vmem_spec),
        scratch_shapes=[
            pltpu.VMEM((11008, LANES), jnp.bfloat16),
            pltpu.VMEM((8, 32, LANES), jnp.bfloat16),
            pltpu.VMEM((8, 8, LANES), jnp.float32),
            pltpu.SemaphoreType.DMA((16,)),
            pltpu.SemaphoreType.DMA((7, 8)),
            pltpu.SemaphoreType.DMA((2, 8)),
            pltpu.SemaphoreType.DMA((2, 8)),
            pltpu.SemaphoreType.DMA,
        ],
        compiler_params=pltpu.CompilerParams(has_side_effects=True),
        name='regroup',
    )(*shards, gain_rows, sumsq)


def adamw_kernel(chunk, me_ref, scale_ref, grad_ref, tail_ref, master_ref, mean_ref, var_ref, *rest):
    new_master, new_mean, new_var, low_ref, wide = rest[-5:]
    me = me_ref[0]
    scale = scale_ref[0]
    shift = lax.rem(4 * me, 16)
    wide[pl.ds(0, STEP_ROWS), :] = grad_ref[...].astype(jnp.float32)
    wide[pl.ds(STEP_ROWS, 16), :] = tail_ref[...].astype(jnp.float32)
    first_row = me * SLAB_ROWS + (chunk * (CHUNK_ROWS // STEP_ROWS) + pl.program_id(0)) * STEP_ROWS

    def body(number, carry):
        base = pl.multiple_of(number * SUB_ROWS, SUB_ROWS)
        rows = pl.ds(base, SUB_ROWS)
        clipped = wide[pl.ds(base + shift, SUB_ROWS), :] * scale
        mean = BETA_ONE * mean_ref[rows, :] + (1.0 - BETA_ONE) * clipped
        var = BETA_TWO * var_ref[rows, :] + (1.0 - BETA_TWO) * clipped * clipped
        new_mean[rows, :] = mean
        new_var[rows, :] = var
        mean_hat = mean / (1.0 - BETA_ONE ** STEP_COUNT)
        var_hat = var / (1.0 - BETA_TWO ** STEP_COUNT)
        row = first_row + base + lax.broadcasted_iota(jnp.int32, (SUB_ROWS, LANES), 0)
        is_gain = (row < 16) | ((row >= GAIN_TWO_ROW) & (row < GAIN_TWO_ROW + 16))
        decays = jnp.where(is_gain, 0.0, WEIGHT_DECAY)
        master = master_ref[rows, :]
        master = master - LEARN_RATE * (mean_hat / (jnp.sqrt(var_hat) + ADAM_EPS) + decays * master)
        new_master[rows, :] = master
        low_ref[rows, :] = master.astype(jnp.bfloat16)
        return carry

    lax.fori_loop(0, STEP_ROWS // SUB_ROWS, body, 0)


def adamw_chunk(chunk, me_vec, scale_vec, grad_rows, state, done):
    steps = CHUNK_ROWS // STEP_ROWS
    first = chunk * steps
    block = pl.BlockSpec((STEP_ROWS, LANES), lambda t, *_: (first + t, 0))
    tail = pl.BlockSpec((16, LANES), lambda t, *_: ((first + t + 1) * (STEP_ROWS // 16), 0))
    any_spec = pl.BlockSpec(memory_space=pl.ANY)
    full = jax.ShapeDtypeStruct((SLAB_ROWS, LANES), jnp.float32)
    return pl.pallas_call(
        functools.partial(adamw_kernel, chunk),
        grid_spec=pltpu.PrefetchScalarGridSpec(
            num_scalar_prefetch=2, grid=(steps,),
            in_specs=[block, tail, block, block, block] + [any_spec] * len(done),
            out_specs=(block, block, block, pl.BlockSpec((STEP_ROWS, LANES), lambda t, *_: (t, 0))),
            scratch_shapes=[pltpu.VMEM((STEP_ROWS + 16, LANES), jnp.float32)]),
        out_shape=(full, full, full, jax.ShapeDtypeStruct((CHUNK_ROWS, LANES), jnp.bfloat16)),
        input_output_aliases={7 + n: n for n in range(len(done))},
        compiler_params=pltpu.CompilerParams(
            dimension_semantics=('arbitrary',), vmem_limit_bytes=48 * 2 ** 20),
        cost_estimate=pl.CostEstimate(flops=30 * CHUNK_ROWS * LANES, bytes_accessed=28 * CHUNK_ROWS * LANES,
                                      transcendentals=0),
        name=f'adamw_{chunk}',
    )(me_vec, scale_vec, grad_rows, grad_rows, *state, *done)


def group_table(chunk):
    table = np.zeros((8, 7, 2), np.int32)
    for slab in range(8):
        start = SLAB_ROWS * slab
        for number, name in enumerate(NAMES):
            size = GROUP_ROWS[name]
            mine = []
            for group in range(ROW_COUNT[name] // size):
                first = ROW_BASE[name] + group * size - start
                stop = first + size
                if not 0 <= first < SLAB_ROWS:
                    continue
                at = NUM_CHUNKS - 1 if stop > SLAB_ROWS else (stop - 1) // CHUNK_ROWS
                if at == chunk:
                    mine.append(group)
            if mine:
                assert mine == list(range(mine[0], mine[-1] + 1))
                table[slab, number] = mine[0], mine[-1] + 1
    return table.reshape(-1)


def unpack_kernel(chunk, table_ref, core_ref, *refs):
    last = chunk == NUM_CHUNKS - 1
    pairs = 1 + (chunk > 0) + last
    sources = refs[:2 * pairs]
    outs, scratch = refs[-7 - 11:-11], refs[-11:]
    stage, carry_in, head_in, wide, out_q, out_w, out_f, load_sem, sem_q, sem_w, sem_f = scratch
    core = core_ref[0]
    slots = 4
    end_row = CARRY_ROWS + SLAB_ROWS - chunk * CHUNK_ROWS

    def load(slab, slot, act):
        def both(pair, owner, rows, target, number):
            chip, parity = owner // 2, lax.rem(owner, 2)
            for which in range(2):
                @pl.when((parity == core) if which == 0 else (parity != core))
                def _():
                    act(pltpu.make_async_copy(sources[2 * pair + which].at[chip, rows, :], target.at[slot],
                                              load_sem.at[slot, number]))
        both(0, slab, pl.ds(0, CHUNK_ROWS), stage, 0)
        if chunk > 0:
            both(1, slab, pl.ds(CHUNK_ROWS - CARRY_ROWS, CARRY_ROWS), carry_in, 1)
        if last:
            @pl.when(slab < 7)
            def _():
                both(2, slab + 1, pl.ds(0, CARRY_ROWS), head_in, 2)

    load(0, 0, lambda copy: copy.start())

    def widen(source, slot, rows, target_row):
        def body(step, carry):
            base = pl.multiple_of(step * 32, 32)
            wide[pl.ds(target_row + base, 32), :] = source[slot, pl.ds(base, 32), :].astype(jnp.float32)
            return carry
        lax.fori_loop(0, rows // 32, body, 0)

    def groups(slab, number, ring, sem, fill, place):
        low = table_ref[(slab * 7 + number) * 2]
        high = table_ref[(slab * 7 + number) * 2 + 1]
        name = NAMES[number]
        origin = ROW_BASE[name] - chunk * CHUNK_ROWS + CARRY_ROWS - slab * SLAB_ROWS

        def copy(group, slot):
            return pltpu.make_async_copy(ring.at[slot], place(group), sem.at[slot])

        def body(group, carry):
            slot = lax.rem(group - low, slots)

            @pl.when(group - low >= slots)
            def _():
                copy(group, slot).wait()
            fill(origin + group * GROUP_ROWS[name], ring, slot)
            copy(group, slot).start()
            return carry
        lax.fori_loop(low, high, body, 0)

        def drain(slot, carry):
            copy(0, slot).wait()
            return carry
        lax.fori_loop(0, jnp.minimum(high - low, slots), drain, 0)

    def fill_rows(row, ring, slot):
        for part in range(8):
            ring[slot, pl.ds(part * 32, 32), :] = wide[pl.ds(row + part * 32, 32), :].astype(jnp.bfloat16)

    def fill_tiles(tiles):
        def fill(row, ring, slot):
            for tile in range(tiles):
                ring[slot, :, pl.ds(tile * LANES, LANES)] = wide[pl.ds(row + tile, 16, stride=tiles), :].astype(jnp.bfloat16)
        return fill

    def slab_step(slab, carry):
        slot = lax.rem(slab, 2)
        load(slab, slot, lambda copy: copy.wait())

        @pl.when(slab < 7)
        def _():
            load(slab + 1, 1 - slot, lambda copy: copy.start())
        widen(stage, slot, CHUNK_ROWS, CARRY_ROWS)
        if chunk > 0:
            widen(carry_in, slot, CARRY_ROWS, 0)
        if last:
            @pl.when(slab < 7)
            def _():
                widen(head_in, slot, CARRY_ROWS, end_row)
        for number in range(3):
            groups(slab, number, out_q, sem_q, fill_rows,
                   lambda group, number=number: outs[number].at[pl.ds(pl.multiple_of(group * 256, 256), 256), :])
        for number, tiles, ring, sem in ((3, 16, out_w, sem_w), (4, 43, out_f, sem_f), (5, 43, out_f, sem_f),
                                         (6, 16, out_w, sem_w)):
            groups(slab, number, ring, sem, fill_tiles(tiles),
                   lambda group, number=number: outs[number].at[pl.ds(pl.multiple_of(group * 16, 16), 16), :])
        return carry

    lax.fori_loop(0, 8, slab_step, 0)


def unpack_chunk(chunk, core_vec, arrays, done):
    any_spec = pl.BlockSpec(memory_space=pl.ANY)
    bf16 = jnp.bfloat16
    shapes = [(32768, LANES)] * 3 + [(2048, 2048), (2048, 5504), (2048, 5504), (5504, 2048)]
    return pl.pallas_call(
        functools.partial(unpack_kernel, chunk),
        grid_spec=pltpu.PrefetchScalarGridSpec(
            num_scalar_prefetch=2, grid=(),
            in_specs=[any_spec] * (len(arrays) + len(done)),
            out_specs=(any_spec,) * 7,
            scratch_shapes=[
                pltpu.VMEM((2, CHUNK_ROWS, LANES), bf16),
                pltpu.VMEM((2, CARRY_ROWS, LANES), bf16),
                pltpu.VMEM((2, CARRY_ROWS, LANES), bf16),
                pltpu.VMEM((CHUNK_ROWS + 2 * CARRY_ROWS, LANES), jnp.float32),
                pltpu.VMEM((4, 256, LANES), bf16),
                pltpu.VMEM((4, 16, 2048), bf16),
                pltpu.VMEM((4, 16, 5504), bf16),
                pltpu.SemaphoreType.DMA((2, 3)),
                pltpu.SemaphoreType.DMA((4,)),
                pltpu.SemaphoreType.DMA((4,)),
                pltpu.SemaphoreType.DMA((4,)),
            ]),
        out_shape=tuple(jax.ShapeDtypeStruct(shape, bf16) for shape in shapes),
        input_output_aliases={2 + len(arrays) + n: n for n in range(len(done))},
        compiler_params=pltpu.CompilerParams(vmem_limit_bytes=40 * 2 ** 20),
        cost_estimate=pl.CostEstimate(flops=10 ** 7, bytes_accessed=4 * 8 * CHUNK_ROWS * LANES, transcendentals=0),
        name=f'unpack_{chunk}',
    )(jnp.asarray(group_table(chunk)), core_vec, *arrays, *done)


def solution(mesh):
    same_core = [[0, 2, 4, 6], [1, 3, 5, 7]]
    partner = [(dev, dev ^ 1) for dev in range(8)]

    def per_device(x_loc, dy_loc, pos_loc, attn_gain, w_query, w_key, w_value, w_out, mlp_gain, w_gate, w_up, w_down, master_loc, mean_loc, var_loc):
        w_list = (attn_gain, w_query, w_key, w_value, w_out, mlp_gain, w_gate, w_up, w_down)
        me = lax.axis_index('dp')
        grad_x, grad_list = local_grads(x_loc, dy_loc, pos_loc, w_list)
        shards = []
        sum_sq = 0.0
        for number in (1, 2, 3, 4, 6, 7, 8):
            shard = lax.psum_scatter(grad_list[number].astype(jnp.bfloat16), 'dp', scatter_dimension=0, tiled=True)
            sum_sq += jnp.sum(jnp.square(shard.astype(jnp.float32)))
            shards.append(shard.reshape(-1, LANES))
        gain_rows = jnp.concatenate([grad_list[0].astype(jnp.bfloat16).reshape(16, LANES),
                                     grad_list[5].astype(jnp.bfloat16).reshape(16, LANES)])
        grad_rows, all_gains, all_sums = regroup(shards, gain_rows, jnp.full((8, LANES), sum_sq / (8 * LANES)))
        gain_sum = jnp.sum(all_gains.astype(jnp.float32), axis=0)
        grad_norm = jnp.sqrt(jnp.sum(all_sums) + jnp.sum(gain_sum * gain_sum)) / 8.0
        clip_scale = jnp.minimum(1.0, 1.0 / (grad_norm + 1e-6))
        gain_low = gain_sum.astype(jnp.bfloat16)
        gain_at = jnp.where(me == 0, 0, jnp.where(me == 2, GAIN_TWO_ROW - frame_start(2), GRAD_ROWS - 16))
        grad_rows = lax.dynamic_update_slice(grad_rows, jnp.where(me == 0, gain_low[:16], gain_low[16:]), (gain_at, 0))
        state = [vec.reshape(SLAB_ROWS, LANES) for vec in (master_loc, mean_loc, var_loc)]
        me_vec = me.astype(jnp.int32)[None]
        scale_vec = (clip_scale / 8.0)[None]
        done = ()
        gathered = []
        for chunk in range(NUM_CHUNKS):
            *done, low = adamw_chunk(chunk, me_vec, scale_vec, grad_rows, state, done)
            own = lax.all_gather(low, 'dp', axis_index_groups=same_core)
            gathered.append((own, lax.ppermute(own, 'dp', partner)))
        new_state = [rows.reshape(-1) for rows in done]
        core_vec = lax.rem(me_vec, 2)
        weights = ()
        for chunk in range(NUM_CHUNKS):
            arrays = gathered[chunk] + (gathered[chunk - 1] if chunk > 0 else ()) + (gathered[0] if chunk == NUM_CHUNKS - 1 else ())
            weights = unpack_chunk(chunk, core_vec, arrays, weights)
        even = core_vec[0] == 0
        gain_outs = []
        for row in (0, GAIN_TWO_ROW):
            slab, local = row // SLAB_ROWS, row % SLAB_ROWS
            chunk, first = local // CHUNK_ROWS, local % CHUNK_ROWS
            mine, other = (pair[slab // 2, first:first + 16] for pair in gathered[chunk])
            gain_outs.append(jnp.where(even, mine, other).reshape(-1))
        return (grad_x, gain_outs[0], weights[0].reshape(w_query.shape), weights[1].reshape(w_key.shape),
                weights[2].reshape(w_value.shape), weights[3].reshape(w_out.shape), gain_outs[1], weights[4],
                weights[5], weights[6], *new_state, grad_norm)

    in_specs = (P('dp'),) * 3 + (P(),) * 9 + (P('dp'),) * 3
    out_specs = (P('dp'),) + (P(),) * 9 + (P('dp'),) * 3 + (P(),)
    return jax.shard_map(per_device, mesh=mesh, in_specs=in_specs, out_specs=out_specs, check_vma=False)
```
